32 devices in a mesh: tm: 4 (over y, x), space: 8 (over z, core).
Axes of the slice: x: 2, y: 2, z: 4, core: 2. Of those that a mesh axis runs over, the one named last changes fastest.
Arguments:
- residual_field: float32 [64, 128, 128, 128], P('tm', 'space'), may hold values from -6 to 6
- eigvec_x: float32 [128, 128], replicated, may hold values from -1 to 1, as said below
- eigvec_y: float32 [128, 128], replicated, may hold values from -1 to 1, as said below
- eigvec_z: float32 [128, 128], replicated, may hold values from -1 to 1, as said below
- eigval_x: float32 [128], replicated, may hold values from 0.0001 to 0.05
- eigval_y: float32 [128], replicated, may hold values from 0.0001 to 0.05
- eigval_z: float32 [128], replicated, may hold values from 0.0001 to 0.05
Outputs:
- update: float32 [64, 128, 128, 128], P('tm', 'space')
The draws below stay inside these ranges and needn't reach their ends.
Inputs may be any that keep to these rules, and one draw needn't show every extreme that they name: `eigvec_x`: an orthogonal matrix. `eigvec_y`: an orthogonal matrix. `eigvec_z`: an orthogonal matrix.
All inputs are finite; a program needn't handle non-finite values.
Results may differ from the reference program's by a relative error of at most 0.00025.
Values sent between devices are 32-bit elements; how exact they have to be, the bound alone decides.
A program may use at most 256 MiB of HBM per device.

```python
import math
import jax
import jax.numpy as jnp
from jax import lax

L = 64
NX = 128
NY = 128
NZ = 128


def orthogonal(key, dimension):

    def reflect(source, matrix):
        vector = jax.random.normal(jax.random.fold_in(key, source), (dimension,), jnp.float32)
        vector = vector / jnp.sqrt(jnp.sum(vector * vector))
        return matrix - 2.0 * jnp.outer(jnp.dot(matrix, vector), vector)
    return lax.fori_loop(0, dimension, reflect, jnp.eye(dimension, dtype=jnp.float32))


def draw_eigvec_x(key, part):
    return orthogonal(jax.random.fold_in(key, 101), NX)


def draw_eigvec_y(key, part):
    return orthogonal(jax.random.fold_in(key, 202), NY)


def draw_eigvec_z(key, part):
    return orthogonal(jax.random.fold_in(key, 303), NZ)


def shard_levels(own_key, dims, cuts, low, top_value):
    gain, own = 1.0, jax.random.fold_in(own_key, 6)
    for position, parts in cuts:
        steps = jnp.exp(jax.random.uniform(jax.random.fold_in(own, position), (parts,), jnp.float32, low / len(cuts), top_value / len(cuts)))
        gain = gain * jnp.repeat(steps, dims[position] // parts).reshape([-1 if axis == position else 1 for axis in range(len(dims))])
    return gain


def gaussian(key, shape, spread, most, pieces=(), held_as=jnp.bfloat16):
    loudness = shard_levels(key, shape, pieces, -0.22, 0.18) if pieces else 1.0
    values = jax.random.normal(key, shape, jnp.float32) * spread * loudness
    return jnp.minimum(jnp.maximum(values, -most), most).astype(held_as)


def setup_inputs(seed: int = 0) -> dict:
    arg_keys = jax.random.split(jax.random.key(seed), 8)
    return {
        "residual_field": gaussian(arg_keys[0], (L, NX, NY, NZ), 1.0, 6.0, ((0, 4), (1, 8)), jnp.float32),
        "eigvec_x": draw_eigvec_x(jax.random.fold_in(arg_keys[7], 71), 0),
        "eigvec_y": draw_eigvec_y(jax.random.fold_in(arg_keys[7], 71), 0),
        "eigvec_z": draw_eigvec_z(jax.random.fold_in(arg_keys[7], 71), 0),
        "eigval_x": jnp.clip(jnp.exp(jax.random.uniform(arg_keys[4], (NX,), jnp.float32, math.log(0.0001), math.log(0.05))), 0.0001, 0.05),
        "eigval_y": jnp.clip(jnp.exp(jax.random.uniform(arg_keys[5], (NY,), jnp.float32, math.log(0.0001), math.log(0.05))), 0.0001, 0.05),
        "eigval_z": jnp.clip(jnp.exp(jax.random.uniform(arg_keys[6], (NZ,), jnp.float32, math.log(0.0001), math.log(0.05))), 0.0001, 0.05),
    }


highest = lax.Precision.HIGHEST
circulant_alpha = 0.01


def spectral_solve(values, shifts, total_steps):
    step_ids = jnp.arange(total_steps, dtype=jnp.int32)
    phases = (step_ids[:, None] * step_ids[None, :]) % total_steps
    angles = (2.0 * math.pi / total_steps) * phases.astype(jnp.float32)
    cosine = jnp.cos(angles)
    sine_table = jnp.sin(angles)
    root_alpha = circulant_alpha ** (1.0 / total_steps)
    powers = root_alpha ** step_ids.astype(jnp.float32)
    flattened = values.reshape(total_steps, -1) * powers[:, None]
    real_part = jnp.dot(cosine, flattened, precision=highest)
    imag_part = -jnp.dot(sine_table, flattened, precision=highest)
    flat_shift = shifts.reshape(1, -1)
    denom_real = 1.0 + flat_shift - root_alpha * cosine[:, 1:2]
    denom_imag = root_alpha * sine_table[:, 1:2]
    modulus = denom_real * denom_real + denom_imag * denom_imag
    quot_real = (real_part * denom_real + imag_part * denom_imag) / modulus
    quot_imag = (imag_part * denom_real - real_part * denom_imag) / modulus
    restored = jnp.dot(cosine, quot_real, precision=highest) - jnp.dot(sine_table, quot_imag, precision=highest)
    restored = restored / (total_steps * powers[:, None])
    return restored.reshape(values.shape)


def reference(residual_field, eigvec_x, eigvec_y, eigvec_z, eigval_x, eigval_y, eigval_z):
    total_steps = residual_field.shape[0]

    def forward_plane(plane):
        plane = jnp.einsum('xyz,zk->xyk', plane, eigvec_z, precision=highest)
        plane = jnp.einsum('xyk,yj->xjk', plane, eigvec_y, precision=highest)
        return jnp.einsum('xjk,xi->ijk', plane, eigvec_x, precision=highest)

    def inverse_plane(plane):
        plane = jnp.einsum('ijk,zk->ijz', plane, eigvec_z, precision=highest)
        plane = jnp.einsum('ijz,yj->iyz', plane, eigvec_y, precision=highest)
        return jnp.einsum('iyz,xi->xyz', plane, eigvec_x, precision=highest)

    coeffs = lax.map(forward_plane, residual_field)
    shift_yz = eigval_y[:, None] + eigval_z[None, :]

    def solve_slab(source):
        slab = lax.dynamic_index_in_dim(coeffs, source, 1, keepdims=False)
        shift_x = lax.dynamic_index_in_dim(eigval_x, source, 0, keepdims=False)
        return spectral_solve(slab, shift_x + shift_yz, total_steps)

    solved = lax.map(solve_slab, jnp.arange(eigval_x.shape[0], dtype=jnp.int32))
    solved = jnp.moveaxis(solved, 0, 1)
    return lax.map(inverse_plane, solved)
```

```python
import functools
import jax
import jax.numpy as jnp
from jax import lax
from jax.experimental import pallas as pl
from jax.experimental.pallas import tpu as pltpu
from jax.sharding import PartitionSpec as P

highest = lax.Precision.HIGHEST
circulant_alpha = 0.01
tile_rows = 8


def halves(a):
    high = a.astype(jnp.bfloat16)
    return high, (a - high.astype(jnp.float32)).astype(jnp.bfloat16)


def stacked(matrix):
    return jnp.concatenate(halves(matrix), axis=0)


def left_product(left, a):
    rows, columns = left.shape[0] // 2, a.shape[1]
    r = jnp.dot(left, jnp.concatenate(halves(a), axis=1), preferred_element_type=jnp.float32)
    return (r[:rows, :columns] + r[rows:, :columns]) + (r[:rows, columns:] + r[rows:, columns:])


def right_product(a, right):
    columns = right.shape[1] // 2
    r = jnp.dot(jnp.concatenate(halves(a), axis=1), right, preferred_element_type=jnp.float32)
    return r[:, :columns] + r[:, columns:]


def power(a, n):
    result = None
    while n:
        if n & 1:
            result = a if result is None else result * a
        a, n = a * a, n >> 1
    return result


def plane_kernel(a_ref, left_ref, right_ref, o_ref):
    left = stacked(left_ref[...])
    right = jnp.concatenate(halves(right_ref[...]), axis=1)
    right = jnp.concatenate([right, right], axis=0)

    def one(x, carry):
        o_ref[0, x] = left_product(left, right_product(a_ref[0, x], right))
        return carry

    lax.fori_loop(0, a_ref.shape[1], one, 0, unroll=4)


def plane_transform(a, left, right):
    steps, rows, size_y, size_z = a.shape
    block = pl.BlockSpec((1, rows, size_y, size_z), lambda t: (t, 0, 0, 0))
    whole = lambda m: pl.BlockSpec(m.shape, lambda t: (0, 0))
    return pl.pallas_call(
        plane_kernel,
        grid=(steps,),
        in_specs=[block, whole(left), whole(right)],
        out_specs=block,
        out_shape=jax.ShapeDtypeStruct(a.shape, jnp.float32),
        compiler_params=pltpu.CompilerParams(vmem_limit_bytes=60 * 2**20),
    )(a, left, right)


def step_groups(steps):
    if steps < 8:
        return [(0, steps)]
    return [(0, 1), (1, 3), (4, steps - 4)]


def reversed_groups(groups):
    steps = sum(count for _, count in groups)
    return [(steps - start - count, count) for start, count in reversed(groups)]


def fused_kernel(
    space_count, time_count, chunks,
    in_ref, vx_ref, vy_ref, vz_ref, ex_ref, ey_ref, ez_ref, out_ref,
    send, recv, fins, entry, ex, shift,
    load_sem, own_in, own_out, go_send, go_recv, back_send, back_recv, st_send, st_recv,
):
    steps, rows, band_rows = recv.shape[2], recv.shape[3], recv.shape[4]
    size_x, size_z = fins.shape[3], fins.shape[4]
    size_y = vy_ref.shape[0]
    band = band_rows * chunks
    me = lax.axis_index("space")
    position = lax.axis_index("tm")
    small_first = step_groups(steps)
    whole = [(0, steps)]
    go_groups = [(c, *g) for c in range(chunks) for g in (small_first if c == 0 else whole)]
    back_groups = [
        (c, *g)
        for c in range(chunks)
        for g in (reversed_groups(small_first) if c == chunks - 1 else whole)
    ]

    def peer_of(k):
        return lax.rem(me + k, space_count)

    def timer_of(k):
        return lax.rem(position + k, time_count)

    def columns(owner, c):
        return pl.ds(pl.multiple_of(owner * band + c * band_rows, tile_rows), band_rows)

    def go(g, peer, slot):
        c, start, count = go_groups[g]
        return pltpu.make_async_remote_copy(
            src_ref=send.at[pl.ds(start, count), :, columns(peer, c), :],
            dst_ref=recv.at[c, slot, pl.ds(start, count)],
            send_sem=go_send.at[g, peer],
            recv_sem=go_recv.at[g, slot],
            device_id={"space": peer},
            device_id_type=pl.DeviceIdType.MESH,
        )

    def back(g, peer, slot):
        c, start, count = back_groups[g]
        return pltpu.make_async_remote_copy(
            src_ref=recv.at[c, peer, pl.ds(start, count)],
            dst_ref=out_ref.at[pl.ds(start, count), :, columns(slot, c), :],
            send_sem=back_send.at[g, peer],
            recv_sem=back_recv.at[g, slot],
            device_id={"space": peer},
            device_id_type=pl.DeviceIdType.MESH,
        )

    def final(c, peer, owner):
        return pltpu.make_async_remote_copy(
            src_ref=fins.at[c, owner],
            dst_ref=fins.at[c, owner],
            send_sem=st_send.at[c, peer],
            recv_sem=st_recv.at[c, owner],
            device_id={"tm": peer},
            device_id_type=pl.DeviceIdType.MESH,
        )

    def take_own(g):
        c, start, count = go_groups[g]
        return pltpu.make_async_copy(
            send.at[pl.ds(start, count), :, columns(me, c), :],
            recv.at[c, me, pl.ds(start, count)],
            own_in.at[g],
        )

    def give_own(g):
        c, start, count = back_groups[g]
        return pltpu.make_async_copy(
            recv.at[c, me, pl.ds(start, count)],
            out_ref.at[pl.ds(start, count), :, columns(me, c), :],
            own_out.at[g],
        )

    def load_step(t):
        return pltpu.make_async_copy(in_ref.at[t], send.at[t], load_sem.at[t])

    def start_load(t, carry):
        load_step(t).start()
        return carry

    lax.fori_loop(0, steps, start_load, 0)

    barrier = pltpu.get_barrier_semaphore()
    for k in range(1, space_count):
        pl.semaphore_signal(
            barrier, inc=1, device_id={"space": peer_of(k)}, device_id_type=pl.DeviceIdType.MESH
        )
    for k in range(1, time_count):
        pl.semaphore_signal(
            barrier, inc=1, device_id={"tm": timer_of(k)}, device_id_type=pl.DeviceIdType.MESH
        )

    middle = space_count // 2
    offsets = sorted(range(1, space_count), key=lambda k: abs(k - middle))

    def plane_loop(ref, start, count, left, right, arrived):
        def one_step(t, carry):
            arrived(t)

            def one(x, carry):
                ref[t, x] = left_product(left, right_product(ref[t, x], right))
                return carry

            return lax.fori_loop(0, rows, one, carry, unroll=4)

        lax.fori_loop(start, start + count, one_step, 0)

    def right_factor(matrix):
        both = jnp.concatenate(halves(matrix), axis=1)
        return jnp.concatenate([both, both], axis=0)

    left = stacked(vy_ref[...].T)
    right = right_factor(vz_ref[...])
    for g, (c, start, count) in enumerate(go_groups):
        if c == 0:
            plane_loop(send, start, count, left, right, lambda t: load_step(t).wait())
        if g == 0:
            pl.semaphore_wait(barrier, space_count + time_count - 2)
        for k in offsets:
            go(g, peer_of(k), me).start()
        take_own(g).start()

    ex[...] = jnp.broadcast_to(ex_ref[...], (size_z, size_x)).T
    shift[...] = jnp.broadcast_to(ey_ref[...], (size_z, size_y)).T + ez_ref[...]
    left = stacked(vx_ref[...].T)
    left_back = stacked(vx_ref[...])

    def load(c, t, j):
        parts = [
            recv.at[c, s, t].reshape(rows * band_rows, size_z)[pl.ds(j, rows, stride=band_rows), :]
            for s in range(space_count)
        ]
        return jnp.concatenate(parts, axis=0)

    def store(c, t, j, value):
        for s in range(space_count):
            view = recv.at[c, s, t].reshape(rows * band_rows, size_z)
            view[pl.ds(j, rows, stride=band_rows), :] = value[s * rows : (s + 1) * rows]

    def damping_of(c, j):
        row = shift[pl.ds(me * band + c * band_rows + j, 1), :]
        return 1.0 / (1.0 + (ex[...] + row))

    for c in range(chunks):
        for g, (of, start, count) in enumerate(go_groups):
            if of != c:
                continue
            for k in offsets:
                go(g, peer_of(k), peer_of(k)).wait_recv()
            take_own(g).wait()

            def forward_mode(j, carry, c=c, start=start, count=count):
                damping = damping_of(c, j)

                def forward(t, state):
                    state = damping * (state + left_product(left, load(c, t, j)))
                    store(c, t, j, state)
                    return state

                first = jnp.zeros_like(damping) if start == 0 else fins[c, position, j]
                fins[c, position, j] = lax.fori_loop(
                    start, start + count, forward, first, unroll=2 if count % 2 == 0 else 1
                )
                return carry

            lax.fori_loop(0, band_rows, forward_mode, 0)
        for k in range(1, time_count):
            final(c, timer_of(k), position).start()
        for k in range(1, time_count):
            final(c, timer_of(k), timer_of(k)).wait_recv()
        for g, (of, start, count) in enumerate(back_groups):
            if of != c:
                continue

            def inverse_mode(j, carry, c=c, start=start, count=count):
                damping = damping_of(c, j)
                if start == 0:
                    block_decay = power(damping, steps)
                    overall = fins[c, 0, j]
                    for p in range(1, time_count):
                        overall = block_decay * overall + fins[c, p, j]
                    incoming = (circulant_alpha * overall) / (
                        1.0 - circulant_alpha * power(block_decay, time_count)
                    )
                    for p in range(time_count - 1):
                        incoming = jnp.where(
                            p < position, block_decay * incoming + fins[c, p, j], incoming
                        )
                else:
                    incoming = entry[j]

                def inverse(t, incoming):
                    incoming = damping * incoming
                    store(c, t, j, left_product(left_back, load(c, t, j) + incoming))
                    return incoming

                entry[j] = lax.fori_loop(
                    start, start + count, inverse, incoming, unroll=2 if count % 2 == 0 else 1
                )
                return carry

            lax.fori_loop(0, band_rows, inverse_mode, 0)
            for k in offsets:
                back(g, peer_of(k), me).start()
            give_own(g).start()

    left = stacked(vy_ref[...])
    right = right_factor(vz_ref[...].T)
    for g, (c, start, count) in enumerate(back_groups):
        for k in offsets:
            back(g, peer_of(k), peer_of(k)).wait_recv()
        give_own(g).wait()
        if c == chunks - 1:
            plane_loop(out_ref, start, count, left, right, lambda t: None)

    for c in range(chunks):
        for k in range(1, time_count):
            final(c, timer_of(k), position).wait_send()
    for g in range(len(go_groups)):
        for k in offsets:
            go(g, peer_of(k), me).wait_send()
    for g in range(len(back_groups)):
        for k in offsets:
            back(g, peer_of(k), me).wait_send()


def chunk_count(band):
    return 2 if band % (2 * tile_rows) == 0 else 1


def fused_solve(field, eigvec_x, eigvec_y, eigvec_z, eigval_x, eigval_y, eigval_z):
    space_count = lax.axis_size("space")
    time_count = lax.axis_size("tm")
    steps, rows, size_y, size_z = field.shape
    band = size_y // space_count
    chunks = chunk_count(band)
    band_rows = band // chunks
    size_x = rows * space_count
    messages = chunks - 1 + len(step_groups(steps))
    vmem = pl.BlockSpec(memory_space=pltpu.VMEM)
    dma = pltpu.SemaphoreType.DMA
    f32 = jnp.float32
    return pl.pallas_call(
        functools.partial(fused_kernel, space_count, time_count, chunks),
        in_specs=[pl.BlockSpec(memory_space=pl.ANY)] + [vmem] * 6,
        out_specs=vmem,
        out_shape=pltpu.VMEM(field.shape, f32),
        scratch_shapes=[
            pltpu.VMEM(field.shape, f32),
            pltpu.VMEM((chunks, space_count, steps, rows, band_rows, size_z), f32),
            pltpu.VMEM((chunks, time_count, band_rows, size_x, size_z), f32),
            pltpu.VMEM((band_rows, size_x, size_z), f32),
            pltpu.VMEM((size_x, size_z), f32),
            pltpu.VMEM((size_y, size_z), f32),
            dma((steps,)),
            dma((messages,)),
            dma((messages,)),
            dma((messages, space_count)),
            dma((messages, space_count)),
            dma((messages, space_count)),
            dma((messages, space_count)),
            dma((chunks, time_count)),
            dma((chunks, time_count)),
        ],
        compiler_params=pltpu.CompilerParams(
            collective_id=0, has_side_effects=True, vmem_limit_bytes=44 * 2**20
        ),
    )(
        field,
        eigvec_x,
        eigvec_y,
        eigvec_z,
        eigval_x.reshape(1, -1),
        eigval_y.reshape(1, -1),
        eigval_z.reshape(1, -1),
    )


def entering(part, axis, combine, identity):
    place = lax.axis_index(axis)
    gathered = jax.tree.map(lambda a: lax.all_gather(a, axis), part)
    state = jax.tree.map(lambda a, e: jnp.zeros_like(a) + jnp.asarray(e, a.dtype), part, identity)

    def one(step, state):
        return combine(
            state, jax.tree.map(lambda a: lax.dynamic_index_in_dim(a, step, 0, False), gathered)
        )

    return lax.fori_loop(0, place, one, state)


def recurrence_solve(values, shifts, time_count):
    steps_local = values.shape[0]
    damping = 1.0 / (1.0 + shifts)

    def advance(running, step_row):
        running = damping * (running + step_row)
        return (running, running)

    final_state, partial_value = lax.scan(advance, jnp.zeros_like(shifts), values)
    block_decay = damping**steps_local
    position = lax.axis_index("tm")

    def compose(early_map, late_map):
        return (early_map[0] * late_map[0], late_map[0] * early_map[1] + late_map[1])

    lead_power, offset = entering(
        (block_decay, final_state), "tm", compose, (jnp.ones_like(shifts), jnp.zeros_like(shifts))
    )
    tail_power = jnp.power(block_decay, (time_count - 1 - position).astype(jnp.float32))
    overall = lax.psum(tail_power * final_state, "tm")
    start_value = circulant_alpha * overall / (1.0 - circulant_alpha * block_decay**time_count)
    incoming = lead_power * start_value + offset
    exponents = jnp.arange(1, steps_local + 1, dtype=jnp.int32).astype(jnp.float32)
    powers = jnp.power(damping[None], exponents[:, None, None])
    return partial_value + powers * incoming[None]


def narrow_solve(planes, eigvec_x, eigval_x, shift_yz, time_count):
    steps_local, rows_x, size_y, size_z = planes.shape
    planes = planes.reshape(steps_local, rows_x, size_y * size_z)
    x_lines = lax.all_to_all(planes, "space", split_axis=2, concat_axis=1, tiled=True)
    x_lines = jnp.einsum("txm,xi->tim", x_lines, eigvec_x, precision=highest)
    shifts = eigval_x[:, None] + shift_yz.reshape(1, -1)
    x_lines = recurrence_solve(x_lines, shifts, time_count)
    x_lines = jnp.einsum("tim,xi->txm", x_lines, eigvec_x, precision=highest)
    planes = lax.all_to_all(x_lines, "space", split_axis=1, concat_axis=2, tiled=True)
    return planes.reshape(steps_local, rows_x, size_y, size_z)


def fits(field, space_count, time_count):
    steps, rows, size_y, size_z = field.shape
    band = size_y // space_count
    if band % tile_rows or rows % tile_rows:
        return False
    states = (time_count + 1) * band * rows * space_count * size_z
    return 4 * (3 * field.size + states) < 60 * 2**20


def shards(residual_field, eigvec_x, eigvec_y, eigvec_z, eigval_x, eigval_y, eigval_z):
    size_y = residual_field.shape[2]
    space_count = lax.axis_size("space")
    time_count = lax.axis_size("tm")
    if fits(residual_field, space_count, time_count):
        return fused_solve(
            residual_field, eigvec_x, eigvec_y, eigvec_z, eigval_x, eigval_y, eigval_z
        )
    planes = plane_transform(residual_field, eigvec_y.T, eigvec_z)
    band = size_y // space_count
    shift_y = lax.dynamic_slice_in_dim(eigval_y, lax.axis_index("space") * band, band, 0)
    shift_yz = shift_y[:, None] + eigval_z[None, :]
    planes = narrow_solve(planes, eigvec_x, eigval_x, shift_yz, time_count)
    return plane_transform(planes, eigvec_y, eigvec_z.T)


def solution(mesh):
    placed = (P("tm", "space", None, None), P(), P(), P(), P(), P(), P())
    return jax.shard_map(
        shards, mesh=mesh, in_specs=placed, out_specs=P("tm", "space", None, None), check_vma=False
    )
```

```python
import functools
import jax
import jax.numpy as jnp
from jax import lax
from jax.experimental import pallas as pl
from jax.experimental.pallas import tpu as pltpu
from jax.sharding import PartitionSpec as P

highest = lax.Precision.HIGHEST
circulant_alpha = 0.01
tile_rows = 8


def halves(a):
    high = a.astype(jnp.bfloat16)
    return high, (a - high.astype(jnp.float32)).astype(jnp.bfloat16)


def stacked(matrix):
    return jnp.concatenate(halves(matrix), axis=0)


def left_product(left, a):
    rows, columns = left.shape[0] // 2, a.shape[1]
    r = jnp.dot(left, jnp.concatenate(halves(a), axis=1), preferred_element_type=jnp.float32)
    return (r[:rows, :columns] + r[rows:, :columns]) + (r[:rows, columns:] + r[rows:, columns:])


def right_product(a, right):
    columns = right.shape[1] // 2
    r = jnp.dot(jnp.concatenate(halves(a), axis=1), right, preferred_element_type=jnp.float32)
    return r[:, :columns] + r[:, columns:]


def power(a, n):
    result = None
    while n:
        if n & 1:
            result = a if result is None else result * a
        a, n = a * a, n >> 1
    return result


def plane_kernel(a_ref, left_ref, right_ref, o_ref):
    left = stacked(left_ref[...])
    right = jnp.concatenate(halves(right_ref[...]), axis=1)
    right = jnp.concatenate([right, right], axis=0)

    def one(x, carry):
        o_ref[0, x] = left_product(left, right_product(a_ref[0, x], right))
        return carry

    lax.fori_loop(0, a_ref.shape[1], one, 0, unroll=4)


def plane_transform(a, left, right):
    steps, rows, size_y, size_z = a.shape
    block = pl.BlockSpec((1, rows, size_y, size_z), lambda t: (t, 0, 0, 0))
    whole = lambda m: pl.BlockSpec(m.shape, lambda t: (0, 0))
    return pl.pallas_call(
        plane_kernel,
        grid=(steps,),
        in_specs=[block, whole(left), whole(right)],
        out_specs=block,
        out_shape=jax.ShapeDtypeStruct(a.shape, jnp.float32),
        compiler_params=pltpu.CompilerParams(vmem_limit_bytes=60 * 2**20),
    )(a, left, right)


def spans(sizes):
    starts = [sum(sizes[:i]) for i in range(len(sizes))]
    return list(zip(starts, sizes))


def growing(total):
    if total % 256:
        return [total]
    return [total // 64, 3 * total // 64, 12 * total // 64, 48 * total // 64]


def shrinking(total):
    sizes = []
    while total > 4 and total % 8 == 0:
        total //= 2
        sizes.append(total)
    return sizes + [total]


def messages(chunks, total):
    outward = [(0, *s) for s in spans(growing(total))]
    outward += [(c, 0, total) for c in range(1, chunks)]
    homeward = [(c, 0, total) for c in range(chunks - 1)]
    homeward += [(chunks - 1, *s) for s in spans(shrinking(total))]
    return outward, homeward


def fused_kernel(
    space_count, time_count, chunks, rows,
    in_ref, vx_ref, vy_ref, vz_ref, ex_ref, ey_ref, ez_ref, out_ref,
    send, recv, fins, matrices, ex, shift,
    load_sem, matrix_sem, own_in, own_out,
    go_send, go_recv, back_send, back_recv, st_send, st_recv,
):
    total, band_rows = recv.shape[2], recv.shape[3]
    size_x, size_z = fins.shape[3], fins.shape[4]
    size_y = vy_ref.shape[0]
    steps = total // rows
    band = band_rows * chunks
    me = lax.axis_index("space")
    position = lax.axis_index("tm")
    outward, homeward = messages(chunks, total)
    middle = space_count // 2
    offsets = sorted(range(1, space_count), key=lambda k: abs(k - middle))

    def peer_of(k):
        return lax.rem(me + k, space_count)

    def timer_of(k):
        return lax.rem(position + k, time_count)

    def columns(owner, c):
        return pl.ds(pl.multiple_of(owner * band + c * band_rows, tile_rows), band_rows)

    def go(g, peer, slot):
        c, start, count = outward[g]
        return pltpu.make_async_remote_copy(
            src_ref=send.at[pl.ds(start, count), columns(peer, c), :],
            dst_ref=recv.at[c, slot, pl.ds(start, count)],
            send_sem=go_send.at[g, peer],
            recv_sem=go_recv.at[g, slot],
            device_id={"space": peer},
            device_id_type=pl.DeviceIdType.MESH,
        )

    def back(g, peer, slot):
        c, start, count = homeward[g]
        return pltpu.make_async_remote_copy(
            src_ref=recv.at[c, peer, pl.ds(start, count)],
            dst_ref=out_ref.at[pl.ds(start, count), columns(slot, c), :],
            send_sem=back_send.at[g, peer],
            recv_sem=back_recv.at[g, slot],
            device_id={"space": peer},
            device_id_type=pl.DeviceIdType.MESH,
        )

    def final(c, peer, owner):
        return pltpu.make_async_remote_copy(
            src_ref=fins.at[c, owner],
            dst_ref=fins.at[c, owner],
            send_sem=st_send.at[c, peer],
            recv_sem=st_recv.at[c, owner],
            device_id={"tm": peer},
            device_id_type=pl.DeviceIdType.MESH,
        )

    def take_own(g):
        c, start, count = outward[g]
        return pltpu.make_async_copy(
            send.at[pl.ds(start, count), columns(me, c), :],
            recv.at[c, me, pl.ds(start, count)],
            own_in.at[g],
        )

    def give_own(g):
        c, start, count = homeward[g]
        return pltpu.make_async_copy(
            recv.at[c, me, pl.ds(start, count)],
            out_ref.at[pl.ds(start, count), columns(me, c), :],
            own_out.at[g],
        )

    loads = [
        pltpu.make_async_copy(
            in_ref.at[pl.ds(start, count)], send.at[pl.ds(start, count)], load_sem.at[g]
        )
        for g, (start, count) in enumerate(spans(growing(total)))
    ]
    fetches = [
        pltpu.make_async_copy(ref, matrices.at[i], matrix_sem.at[i])
        for i, ref in enumerate((vz_ref, vy_ref, vx_ref))
    ]
    barrier = pltpu.get_barrier_semaphore()
    for k in range(1, space_count):
        pl.semaphore_signal(
            barrier, inc=1, device_id={"space": peer_of(k)}, device_id_type=pl.DeviceIdType.MESH
        )
    for k in range(1, time_count):
        pl.semaphore_signal(
            barrier, inc=1, device_id={"tm": timer_of(k)}, device_id_type=pl.DeviceIdType.MESH
        )
    for copy in fetches[:2] + loads + fetches[2:]:
        copy.start()

    def transform_planes(ref, start, count, left, right):
        def one(u, carry):
            ref[u] = left_product(left, right_product(ref[u], right))
            return carry

        lax.fori_loop(start, start + count, one, 0, unroll=4)

    def right_factor(matrix):
        both = jnp.concatenate(halves(matrix), axis=1)
        return jnp.concatenate([both, both], axis=0)

    fetches[0].wait()
    right = right_factor(matrices[0])
    fetches[1].wait()
    left = stacked(matrices[1].T)
    for g, (c, start, count) in enumerate(outward):
        if c == 0:
            loads[g].wait()
            transform_planes(send, start, count, left, right)
        if g == 0:
            pl.semaphore_wait(barrier, space_count + time_count - 2)
        for k in offsets:
            go(g, peer_of(k), me).start()
        take_own(g).start()

    ex[...] = jnp.broadcast_to(ex_ref[...], (size_z, size_x)).T
    shift[...] = jnp.broadcast_to(ey_ref[...], (size_z, size_y)).T + ez_ref[...]
    fetches[2].wait()
    left = stacked(matrices[2].T)
    left_back = stacked(matrices[2])

    def view(c, s, t):
        return recv.at[c, s, pl.ds(t * rows, rows)].reshape(rows * band_rows, size_z)

    def load(c, t, j):
        parts = [view(c, s, t)[pl.ds(j, rows, stride=band_rows), :] for s in range(space_count)]
        return jnp.concatenate(parts, axis=0)

    def store(c, t, j, value):
        for s in range(space_count):
            view(c, s, t)[pl.ds(j, rows, stride=band_rows), :] = value[s * rows : (s + 1) * rows]

    def damping_of(c, j):
        row = shift[pl.ds(me * band + c * band_rows + j, 1), :]
        return 1.0 / (1.0 + (ex[...] + row))

    for c in range(chunks):
        for g in range(len(outward)):
            if outward[g][0] == c:
                for k in offsets:
                    go(g, peer_of(k), peer_of(k)).wait_recv()
                take_own(g).wait()

        def forward_mode(j, carry, c=c):
            damping = damping_of(c, j)

            def forward(t, state):
                state = damping * (state + left_product(left, load(c, t, j)))
                store(c, t, j, state)
                return state

            fins[c, position, j] = lax.fori_loop(
                0, steps, forward, jnp.zeros_like(damping), unroll=2
            )
            return carry

        lax.fori_loop(0, band_rows, forward_mode, 0)
        for k in range(1, time_count):
            final(c, timer_of(k), position).start()
        for k in range(1, time_count):
            final(c, timer_of(k), timer_of(k)).wait_recv()

        def inverse_mode(j, carry, c=c):
            damping = damping_of(c, j)
            block_decay = power(damping, steps)
            overall = fins[c, 0, j]
            for p in range(1, time_count):
                overall = block_decay * overall + fins[c, p, j]
            incoming = (circulant_alpha * overall) / (
                1.0 - circulant_alpha * power(block_decay, time_count)
            )
            for p in range(time_count - 1):
                incoming = jnp.where(
                    p < position, block_decay * incoming + fins[c, p, j], incoming
                )

            def inverse(t, incoming):
                incoming = damping * incoming
                store(c, t, j, left_product(left_back, load(c, t, j) + incoming))
                return incoming

            lax.fori_loop(0, steps, inverse, incoming, unroll=2)
            return carry

        lax.fori_loop(0, band_rows, inverse_mode, 0)
        for g in range(len(homeward)):
            if homeward[g][0] == c:
                for k in offsets:
                    back(g, peer_of(k), me).start()
                give_own(g).start()

    left = stacked(matrices[1])
    right = right_factor(matrices[0].T)
    for g, (c, start, count) in enumerate(homeward):
        for k in offsets:
            back(g, peer_of(k), peer_of(k)).wait_recv()
        give_own(g).wait()
        if c == chunks - 1:
            transform_planes(out_ref, start, count, left, right)

    for c in range(chunks):
        for k in range(1, time_count):
            final(c, timer_of(k), position).wait_send()
    for g in range(len(outward)):
        for k in offsets:
            go(g, peer_of(k), me).wait_send()
    for g in range(len(homeward)):
        for k in offsets:
            back(g, peer_of(k), me).wait_send()


def fused_solve(field, eigvec_x, eigvec_y, eigvec_z, eigval_x, eigval_y, eigval_z):
    space_count = lax.axis_size("space")
    time_count = lax.axis_size("tm")
    steps, rows, size_y, size_z = field.shape
    planes = field.reshape(steps * rows, size_y, size_z)
    band = size_y // space_count
    chunks = 2 if band % (2 * tile_rows) == 0 else 1
    band_rows = band // chunks
    size_x = rows * space_count
    outward, homeward = messages(chunks, steps * rows)
    vmem = pl.BlockSpec(memory_space=pltpu.VMEM)
    hbm = pl.BlockSpec(memory_space=pl.ANY)
    dma = pltpu.SemaphoreType.DMA
    f32 = jnp.float32
    update = pl.pallas_call(
        functools.partial(fused_kernel, space_count, time_count, chunks, rows),
        in_specs=[hbm] * 4 + [vmem] * 3,
        out_specs=vmem,
        out_shape=pltpu.VMEM(planes.shape, f32),
        scratch_shapes=[
            pltpu.VMEM(planes.shape, f32),
            pltpu.VMEM((chunks, space_count, steps * rows, band_rows, size_z), f32),
            pltpu.VMEM((chunks, time_count, band_rows, size_x, size_z), f32),
            pltpu.VMEM((3, size_y, size_z), f32),
            pltpu.VMEM((size_x, size_z), f32),
            pltpu.VMEM((size_y, size_z), f32),
            dma((len(growing(steps * rows)),)),
            dma((3,)),
            dma((len(outward),)),
            dma((len(homeward),)),
            dma((len(outward), space_count)),
            dma((len(outward), space_count)),
            dma((len(homeward), space_count)),
            dma((len(homeward), space_count)),
            dma((chunks, time_count)),
            dma((chunks, time_count)),
        ],
        compiler_params=pltpu.CompilerParams(
            collective_id=0, has_side_effects=True, vmem_limit_bytes=44 * 2**20
        ),
    )(
        planes,
        eigvec_x,
        eigvec_y,
        eigvec_z,
        eigval_x.reshape(1, -1),
        eigval_y.reshape(1, -1),
        eigval_z.reshape(1, -1),
    )
    return update.reshape(field.shape)


def entering(part, axis, combine, identity):
    place = lax.axis_index(axis)
    gathered = jax.tree.map(lambda a: lax.all_gather(a, axis), part)
    state = jax.tree.map(lambda a, e: jnp.zeros_like(a) + jnp.asarray(e, a.dtype), part, identity)

    def one(step, state):
        return combine(
            state, jax.tree.map(lambda a: lax.dynamic_index_in_dim(a, step, 0, False), gathered)
        )

    return lax.fori_loop(0, place, one, state)


def recurrence_solve(values, shifts, time_count):
    steps_local = values.shape[0]
    damping = 1.0 / (1.0 + shifts)

    def advance(running, step_row):
        running = damping * (running + step_row)
        return (running, running)

    final_state, partial_value = lax.scan(advance, jnp.zeros_like(shifts), values)
    block_decay = damping**steps_local
    position = lax.axis_index("tm")

    def compose(early_map, late_map):
        return (early_map[0] * late_map[0], late_map[0] * early_map[1] + late_map[1])

    lead_power, offset = entering(
        (block_decay, final_state), "tm", compose, (jnp.ones_like(shifts), jnp.zeros_like(shifts))
    )
    tail_power = jnp.power(block_decay, (time_count - 1 - position).astype(jnp.float32))
    overall = lax.psum(tail_power * final_state, "tm")
    start_value = circulant_alpha * overall / (1.0 - circulant_alpha * block_decay**time_count)
    incoming = lead_power * start_value + offset
    exponents = jnp.arange(1, steps_local + 1, dtype=jnp.int32).astype(jnp.float32)
    powers = jnp.power(damping[None], exponents[:, None, None])
    return partial_value + powers * incoming[None]


def narrow_solve(planes, eigvec_x, eigval_x, shift_yz, time_count):
    steps_local, rows_x, size_y, size_z = planes.shape
    planes = planes.reshape(steps_local, rows_x, size_y * size_z)
    x_lines = lax.all_to_all(planes, "space", split_axis=2, concat_axis=1, tiled=True)
    x_lines = jnp.einsum("txm,xi->tim", x_lines, eigvec_x, precision=highest)
    shifts = eigval_x[:, None] + shift_yz.reshape(1, -1)
    x_lines = recurrence_solve(x_lines, shifts, time_count)
    x_lines = jnp.einsum("tim,xi->txm", x_lines, eigvec_x, precision=highest)
    planes = lax.all_to_all(x_lines, "space", split_axis=1, concat_axis=2, tiled=True)
    return planes.reshape(steps_local, rows_x, size_y, size_z)


def fits(field, space_count, time_count):
    steps, rows, size_y, size_z = field.shape
    band = size_y // space_count
    if band % tile_rows or rows % tile_rows or not rows * space_count == size_y == size_z:
        return False
    states = (time_count + 1) * band * rows * space_count * size_z
    return 4 * (3 * field.size + states) < 60 * 2**20


def shards(residual_field, eigvec_x, eigvec_y, eigvec_z, eigval_x, eigval_y, eigval_z):
    size_y = residual_field.shape[2]
    space_count = lax.axis_size("space")
    time_count = lax.axis_size("tm")
    if fits(residual_field, space_count, time_count):
        return fused_solve(
            residual_field, eigvec_x, eigvec_y, eigvec_z, eigval_x, eigval_y, eigval_z
        )
    planes = plane_transform(residual_field, eigvec_y.T, eigvec_z)
    band = size_y // space_count
    shift_y = lax.dynamic_slice_in_dim(eigval_y, lax.axis_index("space") * band, band, 0)
    shift_yz = shift_y[:, None] + eigval_z[None, :]
    planes = narrow_solve(planes, eigvec_x, eigval_x, shift_yz, time_count)
    return plane_transform(planes, eigvec_y, eigvec_z.T)


def solution(mesh):
    placed = (P("tm", "space", None, None), P(), P(), P(), P(), P(), P())
    return jax.shard_map(
        shards, mesh=mesh, in_specs=placed, out_specs=P("tm", "space", None, None), check_vma=False
    )
```

```python
import functools
import jax
import jax.numpy as jnp
from jax import lax
from jax.experimental import pallas as pl
from jax.experimental.pallas import tpu as pltpu
from jax.sharding import PartitionSpec as P

highest = lax.Precision.HIGHEST
circulant_alpha = 0.01
tile_rows = 8


def halves(a):
    high = a.astype(jnp.bfloat16)
    return high, (a - high.astype(jnp.float32)).astype(jnp.bfloat16)


def left_factor(matrix):
    return jnp.concatenate(halves(matrix), axis=1)


def right_factor(matrix):
    both = jnp.concatenate(halves(matrix), axis=1)
    return jnp.concatenate([both, both], axis=0)


def left_product(left, a):
    columns = a.shape[1]
    r = jnp.dot(left, right_factor(a), preferred_element_type=jnp.float32)
    return r[:, :columns] + r[:, columns:]


def right_product(a, right):
    columns = right.shape[1] // 2
    r = jnp.dot(jnp.concatenate(halves(a), axis=1), right, preferred_element_type=jnp.float32)
    return r[:, :columns] + r[:, columns:]


def power(a, n):
    result = None
    while n:
        if n & 1:
            result = a if result is None else result * a
        a, n = a * a, n >> 1
    return result


def plane_kernel(a_ref, left_ref, right_ref, o_ref):
    left = left_factor(left_ref[...])
    right = right_factor(right_ref[...])

    def one(x, carry):
        o_ref[0, x] = left_product(left, right_product(a_ref[0, x], right))
        return carry

    lax.fori_loop(0, a_ref.shape[1], one, 0, unroll=4)


def plane_transform(a, left, right):
    steps, rows, size_y, size_z = a.shape
    block = pl.BlockSpec((1, rows, size_y, size_z), lambda t: (t, 0, 0, 0))
    whole = lambda m: pl.BlockSpec(m.shape, lambda t: (0, 0))
    return pl.pallas_call(
        plane_kernel,
        grid=(steps,),
        in_specs=[block, whole(left), whole(right)],
        out_specs=block,
        out_shape=jax.ShapeDtypeStruct(a.shape, jnp.float32),
        compiler_params=pltpu.CompilerParams(vmem_limit_bytes=60 * 2**20),
    )(a, left, right)


def spans(sizes):
    starts = [sum(sizes[:i]) for i in range(len(sizes))]
    return list(zip(starts, sizes))


def growing(total):
    if total % 256:
        return [total]
    return [total // 256 * share for share in (8, 56, 192)]


def shrinking(total):
    if total % 256:
        return [total]
    return [total // 256 * share for share in (160, 64, 24, 8)]


def messages(chunks, total):
    outward = [(0, *s) for s in spans(growing(total))]
    outward += [(c, 0, total) for c in range(1, chunks)]
    homeward = [(c, 0, total) for c in range(chunks - 1)]
    homeward += [(chunks - 1, *s) for s in spans(shrinking(total))]
    return outward, homeward


def fused_kernel(
    space_count, time_count, chunks, rows,
    in_ref, vx_ref, vy_ref, vz_ref, ex_ref, ey_ref, ez_ref, out_ref,
    send, recv, fins, matrices, values, ex, shift,
    load_sem, matrix_sem, value_sem, own_in, own_out,
    go_send, go_recv, back_send, back_recv, st_send, st_recv,
):
    total, band_rows = recv.shape[2], recv.shape[3]
    size_x, size_z = fins.shape[3], fins.shape[4]
    size_y = vy_ref.shape[0]
    steps = total // rows
    band = band_rows * chunks
    me = lax.axis_index("space")
    position = lax.axis_index("tm")
    outward, homeward = messages(chunks, total)
    middle = space_count // 2
    offsets = sorted(range(1, space_count), key=lambda k: abs(k - middle))

    def peer_of(k):
        return lax.rem(me + k, space_count)

    def timer_of(k):
        return lax.rem(position + k, time_count)

    def columns(owner, c):
        return pl.ds(pl.multiple_of(owner * band + c * band_rows, tile_rows), band_rows)

    def go(g, peer, slot):
        c, start, count = outward[g]
        return pltpu.make_async_remote_copy(
            src_ref=send.at[pl.ds(start, count), columns(peer, c), :],
            dst_ref=recv.at[c, slot, pl.ds(start, count)],
            send_sem=go_send.at[g, peer],
            recv_sem=go_recv.at[g, slot],
            device_id={"space": peer},
            device_id_type=pl.DeviceIdType.MESH,
        )

    def back(g, peer, slot):
        c, start, count = homeward[g]
        return pltpu.make_async_remote_copy(
            src_ref=recv.at[c, peer, pl.ds(start, count)],
            dst_ref=out_ref.at[pl.ds(start, count), columns(slot, c), :],
            send_sem=back_send.at[g, peer],
            recv_sem=back_recv.at[g, slot],
            device_id={"space": peer},
            device_id_type=pl.DeviceIdType.MESH,
        )

    def final(c, peer, owner):
        return pltpu.make_async_remote_copy(
            src_ref=fins.at[c, owner],
            dst_ref=fins.at[c, owner],
            send_sem=st_send.at[c, peer],
            recv_sem=st_recv.at[c, owner],
            device_id={"tm": peer},
            device_id_type=pl.DeviceIdType.MESH,
        )

    def take_own(g):
        c, start, count = outward[g]
        return pltpu.make_async_copy(
            send.at[pl.ds(start, count), columns(me, c), :],
            recv.at[c, me, pl.ds(start, count)],
            own_in.at[g],
        )

    def give_own(g):
        c, start, count = homeward[g]
        return pltpu.make_async_copy(
            recv.at[c, me, pl.ds(start, count)],
            out_ref.at[pl.ds(start, count), columns(me, c), :],
            own_out.at[g],
        )

    loads = [
        pltpu.make_async_copy(
            in_ref.at[pl.ds(start, count)], send.at[pl.ds(start, count)], load_sem.at[g]
        )
        for g, (start, count) in enumerate(spans(growing(total)))
    ]
    fetches = [
        pltpu.make_async_copy(ref, matrices.at[i], matrix_sem.at[i])
        for i, ref in enumerate((vz_ref, vy_ref, vx_ref))
    ]
    fetches += [
        pltpu.make_async_copy(ref, values.at[i], value_sem.at[i])
        for i, ref in enumerate((ex_ref, ey_ref, ez_ref))
    ]
    barrier = pltpu.get_barrier_semaphore()
    for k in range(1, space_count):
        pl.semaphore_signal(
            barrier, inc=1, device_id={"space": peer_of(k)}, device_id_type=pl.DeviceIdType.MESH
        )
    for k in range(1, time_count):
        pl.semaphore_signal(
            barrier, inc=1, device_id={"tm": timer_of(k)}, device_id_type=pl.DeviceIdType.MESH
        )
    for copy in fetches[:2] + loads + fetches[2:]:
        copy.start()

    def transform_planes(ref, start, count, left, right):
        def one(u, carry):
            ref[u] = left_product(left, right_product(ref[u], right))
            return carry

        lax.fori_loop(start, start + count, one, 0, unroll=8 if count % 8 == 0 else 1)

    fetches[0].wait()
    right = right_factor(matrices[0])
    fetches[1].wait()
    left = left_factor(matrices[1].T)
    for g, (c, start, count) in enumerate(outward):
        if c == 0:
            loads[g].wait()
            transform_planes(send, start, count, left, right)
        if g == 0:
            pl.semaphore_wait(barrier, space_count + time_count - 2)
        for k in offsets:
            go(g, peer_of(k), me).start()
        take_own(g).start()

    for copy in fetches[2:]:
        copy.wait()
    ex[...] = jnp.broadcast_to(values[0], (size_z, size_x)).T
    shift[...] = jnp.broadcast_to(values[1], (size_z, size_y)).T + values[2]
    left = left_factor(matrices[2].T)
    left_back = left_factor(matrices[2])

    def view(c, s, t):
        return recv.at[c, s, pl.ds(t * rows, rows)].reshape(rows * band_rows, size_z)

    def load(c, t, j):
        parts = [view(c, s, t)[pl.ds(j, rows, stride=band_rows), :] for s in range(space_count)]
        return jnp.concatenate(parts, axis=0)

    def store(c, t, j, value):
        for s in range(space_count):
            view(c, s, t)[pl.ds(j, rows, stride=band_rows), :] = value[s * rows : (s + 1) * rows]

    def damping_of(c, j):
        row = shift[pl.ds(me * band + c * band_rows + j, 1), :]
        return 1.0 / (1.0 + (ex[...] + row))

    for c in range(chunks):
        for g in range(len(outward)):
            if outward[g][0] == c:
                for k in offsets:
                    go(g, peer_of(k), peer_of(k)).wait_recv()
                take_own(g).wait()

        def forward_mode(j, carry, c=c):
            damping = damping_of(c, j)

            def forward(t, state):
                state = damping * (state + left_product(left, load(c, t, j)))
                store(c, t, j, state)
                return state

            fins[c, position, j] = lax.fori_loop(
                0, steps, forward, jnp.zeros_like(damping), unroll=2
            )
            return carry

        lax.fori_loop(0, band_rows, forward_mode, 0)
        for k in range(1, time_count):
            final(c, timer_of(k), position).start()
        for k in range(1, time_count):
            final(c, timer_of(k), timer_of(k)).wait_recv()

        def inverse_mode(j, carry, c=c):
            damping = damping_of(c, j)
            block_decay = power(damping, steps)
            overall = fins[c, 0, j]
            for p in range(1, time_count):
                overall = block_decay * overall + fins[c, p, j]
            incoming = (circulant_alpha * overall) / (
                1.0 - circulant_alpha * power(block_decay, time_count)
            )
            for p in range(time_count - 1):
                incoming = jnp.where(
                    p < position, block_decay * incoming + fins[c, p, j], incoming
                )

            def inverse(t, incoming):
                incoming = damping * incoming
                store(c, t, j, left_product(left_back, load(c, t, j) + incoming))
                return incoming

            lax.fori_loop(0, steps, inverse, incoming, unroll=2)
            return carry

        lax.fori_loop(0, band_rows, inverse_mode, 0)
        for g in range(len(homeward)):
            if homeward[g][0] == c:
                for k in offsets:
                    back(g, peer_of(k), me).start()
                give_own(g).start()

    left = left_factor(matrices[1])
    right = right_factor(matrices[0].T)
    for g, (c, start, count) in enumerate(homeward):
        for k in offsets:
            back(g, peer_of(k), peer_of(k)).wait_recv()
        give_own(g).wait()
        if c == chunks - 1:
            transform_planes(out_ref, start, count, left, right)

    for c in range(chunks):
        for k in range(1, time_count):
            final(c, timer_of(k), position).wait_send()
    for g in range(len(outward)):
        for k in offsets:
            go(g, peer_of(k), me).wait_send()
    for g in range(len(homeward)):
        for k in offsets:
            back(g, peer_of(k), me).wait_send()


def fused_solve(field, eigvec_x, eigvec_y, eigvec_z, eigval_x, eigval_y, eigval_z):
    space_count = lax.axis_size("space")
    time_count = lax.axis_size("tm")
    steps, rows, size_y, size_z = field.shape
    planes = field.reshape(steps * rows, size_y, size_z)
    band = size_y // space_count
    chunks = 2 if band % (2 * tile_rows) == 0 else 1
    band_rows = band // chunks
    size_x = rows * space_count
    outward, homeward = messages(chunks, steps * rows)
    vmem = pl.BlockSpec(memory_space=pltpu.VMEM)
    hbm = pl.BlockSpec(memory_space=pl.ANY)
    dma = pltpu.SemaphoreType.DMA
    f32 = jnp.float32
    update = pl.pallas_call(
        functools.partial(fused_kernel, space_count, time_count, chunks, rows),
        in_specs=[hbm] * 7,
        out_specs=vmem,
        out_shape=pltpu.VMEM(planes.shape, f32),
        scratch_shapes=[
            pltpu.VMEM(planes.shape, f32),
            pltpu.VMEM((chunks, space_count, steps * rows, band_rows, size_z), f32),
            pltpu.VMEM((chunks, time_count, band_rows, size_x, size_z), f32),
            pltpu.VMEM((3, size_y, size_z), f32),
            pltpu.VMEM((3, 1, size_z), f32),
            pltpu.VMEM((size_x, size_z), f32),
            pltpu.VMEM((size_y, size_z), f32),
            dma((len(growing(steps * rows)),)),
            dma((3,)),
            dma((3,)),
            dma((len(outward),)),
            dma((len(homeward),)),
            dma((len(outward), space_count)),
            dma((len(outward), space_count)),
            dma((len(homeward), space_count)),
            dma((len(homeward), space_count)),
            dma((chunks, time_count)),
            dma((chunks, time_count)),
        ],
        compiler_params=pltpu.CompilerParams(
            collective_id=0, has_side_effects=True, vmem_limit_bytes=44 * 2**20
        ),
    )(
        planes,
        eigvec_x,
        eigvec_y,
        eigvec_z,
        eigval_x.reshape(1, -1),
        eigval_y.reshape(1, -1),
        eigval_z.reshape(1, -1),
    )
    return update.reshape(field.shape)


def entering(part, axis, combine, identity):
    place = lax.axis_index(axis)
    gathered = jax.tree.map(lambda a: lax.all_gather(a, axis), part)
    state = jax.tree.map(lambda a, e: jnp.zeros_like(a) + jnp.asarray(e, a.dtype), part, identity)

    def one(step, state):
        return combine(
            state, jax.tree.map(lambda a: lax.dynamic_index_in_dim(a, step, 0, False), gathered)
        )

    return lax.fori_loop(0, place, one, state)


def recurrence_solve(values, shifts, time_count):
    steps_local = values.shape[0]
    damping = 1.0 / (1.0 + shifts)

    def advance(running, step_row):
        running = damping * (running + step_row)
        return (running, running)

    final_state, partial_value = lax.scan(advance, jnp.zeros_like(shifts), values)
    block_decay = damping**steps_local
    position = lax.axis_index("tm")

    def compose(early_map, late_map):
        return (early_map[0] * late_map[0], late_map[0] * early_map[1] + late_map[1])

    lead_power, offset = entering(
        (block_decay, final_state), "tm", compose, (jnp.ones_like(shifts), jnp.zeros_like(shifts))
    )
    tail_power = jnp.power(block_decay, (time_count - 1 - position).astype(jnp.float32))
    overall = lax.psum(tail_power * final_state, "tm")
    start_value = circulant_alpha * overall / (1.0 - circulant_alpha * block_decay**time_count)
    incoming = lead_power * start_value + offset
    exponents = jnp.arange(1, steps_local + 1, dtype=jnp.int32).astype(jnp.float32)
    powers = jnp.power(damping[None], exponents[:, None, None])
    return partial_value + powers * incoming[None]


def narrow_solve(planes, eigvec_x, eigval_x, shift_yz, time_count):
    steps_local, rows_x, size_y, size_z = planes.shape
    planes = planes.reshape(steps_local, rows_x, size_y * size_z)
    x_lines = lax.all_to_all(planes, "space", split_axis=2, concat_axis=1, tiled=True)
    x_lines = jnp.einsum("txm,xi->tim", x_lines, eigvec_x, precision=highest)
    shifts = eigval_x[:, None] + shift_yz.reshape(1, -1)
    x_lines = recurrence_solve(x_lines, shifts, time_count)
    x_lines = jnp.einsum("tim,xi->txm", x_lines, eigvec_x, precision=highest)
    planes = lax.all_to_all(x_lines, "space", split_axis=1, concat_axis=2, tiled=True)
    return planes.reshape(steps_local, rows_x, size_y, size_z)


def fits(field, space_count, time_count):
    steps, rows, size_y, size_z = field.shape
    band = size_y // space_count
    if band % tile_rows or rows % tile_rows or not rows * space_count == size_y == size_z:
        return False
    states = (time_count + 1) * band * rows * space_count * size_z
    return 4 * (3 * field.size + states) < 60 * 2**20


def shards(residual_field, eigvec_x, eigvec_y, eigvec_z, eigval_x, eigval_y, eigval_z):
    size_y = residual_field.shape[2]
    space_count = lax.axis_size("space")
    time_count = lax.axis_size("tm")
    if fits(residual_field, space_count, time_count):
        return fused_solve(
            residual_field, eigvec_x, eigvec_y, eigvec_z, eigval_x, eigval_y, eigval_z
        )
    planes = plane_transform(residual_field, eigvec_y.T, eigvec_z)
    band = size_y // space_count
    shift_y = lax.dynamic_slice_in_dim(eigval_y, lax.axis_index("space") * band, band, 0)
    shift_yz = shift_y[:, None] + eigval_z[None, :]
    planes = narrow_solve(planes, eigvec_x, eigval_x, shift_yz, time_count)
    return plane_transform(planes, eigvec_y, eigvec_z.T)


def solution(mesh):
    placed = (P("tm", "space", None, None), P(), P(), P(), P(), P(), P())
    return jax.shard_map(
        shards, mesh=mesh, in_specs=placed, out_specs=P("tm", "space", None, None), check_vma=False
    )
```

```python
import functools
import jax
import jax.numpy as jnp
from jax import lax
from jax.experimental import pallas as pl
from jax.experimental.pallas import tpu as pltpu
from jax.sharding import PartitionSpec as P

highest = lax.Precision.HIGHEST
circulant_alpha = 0.01
tile_rows = 8


def halves(a):
    high = a.astype(jnp.bfloat16)
    return high, (a - high.astype(jnp.float32)).astype(jnp.bfloat16)


def left_factor(matrix):
    return jnp.concatenate(halves(matrix), axis=1)


def right_factor(matrix):
    both = jnp.concatenate(halves(matrix), axis=1)
    return jnp.concatenate([both, both], axis=0)


def left_product(left, a):
    columns = a.shape[1]
    r = jnp.dot(left, right_factor(a), preferred_element_type=jnp.float32)
    return r[:, :columns] + r[:, columns:]


def right_product(a, right):
    columns = right.shape[1] // 2
    r = jnp.dot(jnp.concatenate(halves(a), axis=1), right, preferred_element_type=jnp.float32)
    return r[:, :columns] + r[:, columns:]


def power(a, n):
    result = None
    while n:
        if n & 1:
            result = a if result is None else result * a
        a, n = a * a, n >> 1
    return result


def plane_kernel(a_ref, left_ref, right_ref, o_ref):
    left = left_factor(left_ref[...])
    right = right_factor(right_ref[...])

    def one(x, carry):
        o_ref[0, x] = left_product(left, right_product(a_ref[0, x], right))
        return carry

    lax.fori_loop(0, a_ref.shape[1], one, 0, unroll=4)


def plane_transform(a, left, right):
    steps, rows, size_y, size_z = a.shape
    block = pl.BlockSpec((1, rows, size_y, size_z), lambda t: (t, 0, 0, 0))
    whole = lambda m: pl.BlockSpec(m.shape, lambda t: (0, 0))
    return pl.pallas_call(
        plane_kernel,
        grid=(steps,),
        in_specs=[block, whole(left), whole(right)],
        out_specs=block,
        out_shape=jax.ShapeDtypeStruct(a.shape, jnp.float32),
        compiler_params=pltpu.CompilerParams(vmem_limit_bytes=60 * 2**20),
    )(a, left, right)


def spans(sizes):
    starts = [sum(sizes[:i]) for i in range(len(sizes))]
    return list(zip(starts, sizes))


def growing(total):
    if total % 256:
        return [total]
    return [total // 256 * share for share in (8, 56, 192)]


def shrinking(total):
    if total % 256:
        return [total]
    return [total // 256 * share for share in (160, 64, 16, 16)]


def transform_planes(source, target, start, count, left, right, shift=0):
    def one(u, carry):
        target[u - shift] = left_product(left, right_product(source[u], right))
        return carry

    lax.fori_loop(start, start + count, one, 0, unroll=8 if count % 8 == 0 else 1)


def messages(chunks, total):
    outward = [(0, *s) for s in spans(growing(total))]
    outward += [(c, 0, total) for c in range(1, chunks)]
    homeward = [(c, 0, total) for c in range(chunks - 1)]
    homeward += [(chunks - 1, *s) for s in spans(shrinking(total))]
    return outward, homeward


def fused_kernel(
    space_count, time_count, chunks, rows,
    in_ref, vx_ref, vy_ref, vz_ref, ex_ref, ey_ref, ez_ref, out_ref,
    send, recv, fins, matrices, values, ex, shift,
    load_sem, matrix_sem, value_sem, own_in, own_out,
    go_send, go_recv, back_send, back_recv, st_send, st_recv,
):
    total, band_rows = recv.shape[2], recv.shape[3]
    size_x, size_z = fins.shape[3], fins.shape[4]
    size_y = vy_ref.shape[0]
    steps = total // rows
    band = band_rows * chunks
    me = lax.axis_index("space")
    position = lax.axis_index("tm")
    outward, homeward = messages(chunks, total)
    middle = space_count // 2
    offsets = sorted(range(1, space_count), key=lambda k: abs(k - middle))

    def peer_of(k):
        return lax.rem(me + k, space_count)

    def timer_of(k):
        return lax.rem(position + k, time_count)

    def columns(owner, c):
        return pl.ds(pl.multiple_of(owner * band + c * band_rows, tile_rows), band_rows)

    def go(g, peer, slot):
        c, start, count = outward[g]
        return pltpu.make_async_remote_copy(
            src_ref=send.at[pl.ds(start, count), columns(peer, c), :],
            dst_ref=recv.at[c, slot, pl.ds(start, count)],
            send_sem=go_send.at[g, peer],
            recv_sem=go_recv.at[g, slot],
            device_id={"space": peer},
            device_id_type=pl.DeviceIdType.MESH,
        )

    def back(g, peer, slot):
        c, start, count = homeward[g]
        return pltpu.make_async_remote_copy(
            src_ref=recv.at[c, peer, pl.ds(start, count)],
            dst_ref=out_ref.at[pl.ds(start, count), columns(slot, c), :],
            send_sem=back_send.at[g, peer],
            recv_sem=back_recv.at[g, slot],
            device_id={"space": peer},
            device_id_type=pl.DeviceIdType.MESH,
        )

    def final(c, peer, owner):
        return pltpu.make_async_remote_copy(
            src_ref=fins.at[c, owner],
            dst_ref=fins.at[c, owner],
            send_sem=st_send.at[c, peer],
            recv_sem=st_recv.at[c, owner],
            device_id={"tm": peer},
            device_id_type=pl.DeviceIdType.MESH,
        )

    def take_own(g):
        c, start, count = outward[g]
        return pltpu.make_async_copy(
            send.at[pl.ds(start, count), columns(me, c), :],
            recv.at[c, me, pl.ds(start, count)],
            own_in.at[g],
        )

    def give_own(g):
        c, start, count = homeward[g]
        return pltpu.make_async_copy(
            recv.at[c, me, pl.ds(start, count)],
            out_ref.at[pl.ds(start, count), columns(me, c), :],
            own_out.at[g],
        )

    loads = [
        pltpu.make_async_copy(
            in_ref.at[pl.ds(start, count)], send.at[pl.ds(start, count)], load_sem.at[g]
        )
        for g, (start, count) in enumerate(spans(growing(total)))
    ]
    fetches = [
        pltpu.make_async_copy(ref, matrices.at[i], matrix_sem.at[i])
        for i, ref in enumerate((vz_ref, vy_ref, vx_ref))
    ]
    fetches += [
        pltpu.make_async_copy(ref, values.at[i], value_sem.at[i])
        for i, ref in enumerate((ex_ref, ey_ref, ez_ref))
    ]
    barrier = pltpu.get_barrier_semaphore()
    for k in range(1, space_count):
        pl.semaphore_signal(
            barrier, inc=1, device_id={"space": peer_of(k)}, device_id_type=pl.DeviceIdType.MESH
        )
    for k in range(1, time_count):
        pl.semaphore_signal(
            barrier, inc=1, device_id={"tm": timer_of(k)}, device_id_type=pl.DeviceIdType.MESH
        )
    for copy in fetches[:2] + loads + fetches[2:]:
        copy.start()

    fetches[0].wait()
    right = right_factor(matrices[0])
    fetches[1].wait()
    left = left_factor(matrices[1].T)
    for g, (c, start, count) in enumerate(outward):
        if c == 0:
            loads[g].wait()
            transform_planes(send, send, start, count, left, right)
        if g == 0:
            pl.semaphore_wait(barrier, space_count + time_count - 2)
        for k in offsets:
            go(g, peer_of(k), me).start()
        take_own(g).start()

    for copy in fetches[2:]:
        copy.wait()
    ex[...] = jnp.broadcast_to(values[0], (size_z, size_x)).T
    shift[...] = jnp.broadcast_to(values[1], (size_z, size_y)).T + values[2]
    left = left_factor(matrices[2].T)
    left_back = left_factor(matrices[2])

    def view(c, s, t):
        return recv.at[c, s, pl.ds(t * rows, rows)].reshape(rows * band_rows, size_z)

    def load(c, t, j):
        parts = [view(c, s, t)[pl.ds(j, rows, stride=band_rows), :] for s in range(space_count)]
        return jnp.concatenate(parts, axis=0)

    def store(c, t, j, value):
        for s in range(space_count):
            view(c, s, t)[pl.ds(j, rows, stride=band_rows), :] = value[s * rows : (s + 1) * rows]

    def damping_of(c, j):
        row = shift[pl.ds(me * band + c * band_rows + j, 1), :]
        return 1.0 / (1.0 + (ex[...] + row))

    for c in range(chunks):
        for g in range(len(outward)):
            if outward[g][0] == c:
                for k in offsets:
                    go(g, peer_of(k), peer_of(k)).wait_recv()
                take_own(g).wait()

        def forward_mode(j, carry, c=c):
            damping = damping_of(c, j)

            def forward(t, state):
                state = damping * (state + left_product(left, load(c, t, j)))
                store(c, t, j, state)
                return state

            fins[c, position, j] = lax.fori_loop(
                0, steps, forward, jnp.zeros_like(damping), unroll=2
            )
            return carry

        lax.fori_loop(0, band_rows, forward_mode, 0)
        for k in range(1, time_count):
            final(c, timer_of(k), position).start()
        for k in range(1, time_count):
            final(c, timer_of(k), timer_of(k)).wait_recv()

        def inverse_mode(j, carry, c=c):
            damping = damping_of(c, j)
            block_decay = power(damping, steps)
            overall = fins[c, 0, j]
            for p in range(1, time_count):
                overall = block_decay * overall + fins[c, p, j]
            incoming = (circulant_alpha * overall) / (
                1.0 - circulant_alpha * power(block_decay, time_count)
            )
            for p in range(time_count - 1):
                incoming = jnp.where(
                    p < position, block_decay * incoming + fins[c, p, j], incoming
                )

            def inverse(t, incoming):
                incoming = damping * incoming
                store(c, t, j, left_product(left_back, load(c, t, j) + incoming))
                return incoming

            lax.fori_loop(0, steps, inverse, incoming, unroll=2)
            return carry

        lax.fori_loop(0, band_rows, inverse_mode, 0)
        for g in range(len(homeward)):
            if homeward[g][0] == c:
                for k in offsets:
                    back(g, peer_of(k), me).start()
                give_own(g).start()

    left = left_factor(matrices[1])
    right = right_factor(matrices[0].T)
    for g, (c, start, count) in enumerate(homeward):
        for k in offsets:
            back(g, peer_of(k), peer_of(k)).wait_recv()
        give_own(g).wait()
        if c == chunks - 1 and g < len(homeward) - 1:
            transform_planes(out_ref, out_ref, start, count, left, right)

    for c in range(chunks):
        for k in range(1, time_count):
            final(c, timer_of(k), position).wait_send()
    for g in range(len(outward)):
        for k in offsets:
            go(g, peer_of(k), me).wait_send()
    for g in range(len(homeward)):
        for k in offsets:
            back(g, peer_of(k), me).wait_send()


def closing_kernel(in_ref, left_ref, right_ref, out_ref, last, sems):
    held = last.shape[0]
    done = in_ref.shape[0] - held
    pieces = sems.shape[0] - 1
    piece = done // pieces
    copies = [
        pltpu.make_async_copy(
            in_ref.at[pl.ds(i * piece, piece)], out_ref.at[pl.ds(i * piece, piece)], sems.at[i]
        )
        for i in range(pieces)
    ]
    for copy in copies:
        copy.start()
    left = left_factor(left_ref[...])
    right = right_factor(right_ref[...].T)
    transform_planes(in_ref, last, done, held, left, right, shift=done)
    copies.append(pltpu.make_async_copy(last, out_ref.at[pl.ds(done, held)], sems.at[pieces]))
    copies[-1].start()
    for copy in copies:
        copy.wait()


def close(planes, left, right):
    vmem = pl.BlockSpec(memory_space=pltpu.VMEM)
    held = shrinking(planes.shape[0])[-1]
    done = planes.shape[0] - held
    pieces = 6 if done % 6 == 0 else 1
    return pl.pallas_call(
        closing_kernel,
        in_specs=[vmem] * 3,
        out_specs=pl.BlockSpec(memory_space=pltpu.HBM),
        out_shape=jax.ShapeDtypeStruct(planes.shape, jnp.float32),
        scratch_shapes=[
            pltpu.VMEM((held, *planes.shape[1:]), jnp.float32),
            pltpu.SemaphoreType.DMA((pieces + 1,)),
        ],
        compiler_params=pltpu.CompilerParams(vmem_limit_bytes=24 * 2**20),
    )(planes, left, right)


def fused_solve(field, eigvec_x, eigvec_y, eigvec_z, eigval_x, eigval_y, eigval_z):
    space_count = lax.axis_size("space")
    time_count = lax.axis_size("tm")
    steps, rows, size_y, size_z = field.shape
    planes = field.reshape(steps * rows, size_y, size_z)
    band = size_y // space_count
    chunks = 2 if band % (2 * tile_rows) == 0 else 1
    band_rows = band // chunks
    size_x = rows * space_count
    outward, homeward = messages(chunks, steps * rows)
    vmem = pl.BlockSpec(memory_space=pltpu.VMEM)
    hbm = pl.BlockSpec(memory_space=pl.ANY)
    dma = pltpu.SemaphoreType.DMA
    f32 = jnp.float32
    update = pl.pallas_call(
        functools.partial(fused_kernel, space_count, time_count, chunks, rows),
        in_specs=[hbm] * 7,
        out_specs=vmem,
        out_shape=pltpu.VMEM(planes.shape, f32),
        scratch_shapes=[
            pltpu.VMEM(planes.shape, f32),
            pltpu.VMEM((chunks, space_count, steps * rows, band_rows, size_z), f32),
            pltpu.VMEM((chunks, time_count, band_rows, size_x, size_z), f32),
            pltpu.VMEM((3, size_y, size_z), f32),
            pltpu.VMEM((3, 1, size_z), f32),
            pltpu.VMEM((size_x, size_z), f32),
            pltpu.VMEM((size_y, size_z), f32),
            dma((len(growing(steps * rows)),)),
            dma((3,)),
            dma((3,)),
            dma((len(outward),)),
            dma((len(homeward),)),
            dma((len(outward), space_count)),
            dma((len(outward), space_count)),
            dma((len(homeward), space_count)),
            dma((len(homeward), space_count)),
            dma((chunks, time_count)),
            dma((chunks, time_count)),
        ],
        compiler_params=pltpu.CompilerParams(
            collective_id=0, has_side_effects=True, vmem_limit_bytes=44 * 2**20
        ),
    )(
        planes,
        eigvec_x,
        eigvec_y,
        eigvec_z,
        eigval_x.reshape(1, -1),
        eigval_y.reshape(1, -1),
        eigval_z.reshape(1, -1),
    )
    return close(update, eigvec_y, eigvec_z).reshape(field.shape)


def entering(part, axis, combine, identity):
    place = lax.axis_index(axis)
    gathered = jax.tree.map(lambda a: lax.all_gather(a, axis), part)
    state = jax.tree.map(lambda a, e: jnp.zeros_like(a) + jnp.asarray(e, a.dtype), part, identity)

    def one(step, state):
        return combine(
            state, jax.tree.map(lambda a: lax.dynamic_index_in_dim(a, step, 0, False), gathered)
        )

    return lax.fori_loop(0, place, one, state)


def recurrence_solve(values, shifts, time_count):
    steps_local = values.shape[0]
    damping = 1.0 / (1.0 + shifts)

    def advance(running, step_row):
        running = damping * (running + step_row)
        return (running, running)

    final_state, partial_value = lax.scan(advance, jnp.zeros_like(shifts), values)
    block_decay = damping**steps_local
    position = lax.axis_index("tm")

    def compose(early_map, late_map):
        return (early_map[0] * late_map[0], late_map[0] * early_map[1] + late_map[1])

    lead_power, offset = entering(
        (block_decay, final_state), "tm", compose, (jnp.ones_like(shifts), jnp.zeros_like(shifts))
    )
    tail_power = jnp.power(block_decay, (time_count - 1 - position).astype(jnp.float32))
    overall = lax.psum(tail_power * final_state, "tm")
    start_value = circulant_alpha * overall / (1.0 - circulant_alpha * block_decay**time_count)
    incoming = lead_power * start_value + offset
    exponents = jnp.arange(1, steps_local + 1, dtype=jnp.int32).astype(jnp.float32)
    powers = jnp.power(damping[None], exponents[:, None, None])
    return partial_value + powers * incoming[None]


def narrow_solve(planes, eigvec_x, eigval_x, shift_yz, time_count):
    steps_local, rows_x, size_y, size_z = planes.shape
    planes = planes.reshape(steps_local, rows_x, size_y * size_z)
    x_lines = lax.all_to_all(planes, "space", split_axis=2, concat_axis=1, tiled=True)
    x_lines = jnp.einsum("txm,xi->tim", x_lines, eigvec_x, precision=highest)
    shifts = eigval_x[:, None] + shift_yz.reshape(1, -1)
    x_lines = recurrence_solve(x_lines, shifts, time_count)
    x_lines = jnp.einsum("tim,xi->txm", x_lines, eigvec_x, precision=highest)
    planes = lax.all_to_all(x_lines, "space", split_axis=1, concat_axis=2, tiled=True)
    return planes.reshape(steps_local, rows_x, size_y, size_z)


def fits(field, space_count, time_count):
    steps, rows, size_y, size_z = field.shape
    band = size_y // space_count
    if band % tile_rows or rows % tile_rows or not rows * space_count == size_y == size_z or steps * rows % 256:
        return False
    states = (time_count + 1) * band * rows * space_count * size_z
    return 4 * (3 * field.size + states) < 60 * 2**20


def shards(residual_field, eigvec_x, eigvec_y, eigvec_z, eigval_x, eigval_y, eigval_z):
    size_y = residual_field.shape[2]
    space_count = lax.axis_size("space")
    time_count = lax.axis_size("tm")
    if fits(residual_field, space_count, time_count):
        return fused_solve(
            residual_field, eigvec_x, eigvec_y, eigvec_z, eigval_x, eigval_y, eigval_z
        )
    planes = plane_transform(residual_field, eigvec_y.T, eigvec_z)
    band = size_y // space_count
    shift_y = lax.dynamic_slice_in_dim(eigval_y, lax.axis_index("space") * band, band, 0)
    shift_yz = shift_y[:, None] + eigval_z[None, :]
    planes = narrow_solve(planes, eigvec_x, eigval_x, shift_yz, time_count)
    return plane_transform(planes, eigvec_y, eigvec_z.T)


def solution(mesh):
    placed = (P("tm", "space", None, None), P(), P(), P(), P(), P(), P())
    return jax.shard_map(
        shards, mesh=mesh, in_specs=placed, out_specs=P("tm", "space", None, None), check_vma=False
    )
```

```python
import functools
import jax
import jax.numpy as jnp
from jax import lax
from jax.experimental import pallas as pl
from jax.experimental.pallas import tpu as pltpu
from jax.sharding import PartitionSpec as P

highest = lax.Precision.HIGHEST
circulant_alpha = 0.01
tile_rows = 8


def halves(a):
    high = a.astype(jnp.bfloat16)
    return high, (a - high.astype(jnp.float32)).astype(jnp.bfloat16)


def left_factor(matrix):
    return jnp.concatenate(halves(matrix), axis=1)


def right_factor(matrix):
    both = jnp.concatenate(halves(matrix), axis=1)
    return jnp.concatenate([both, both], axis=0)


def left_product(left, a):
    columns = a.shape[1]
    r = jnp.dot(left, right_factor(a), preferred_element_type=jnp.float32)
    return r[:, :columns] + r[:, columns:]


def right_product(a, right):
    columns = right.shape[1] // 2
    r = jnp.dot(jnp.concatenate(halves(a), axis=1), right, preferred_element_type=jnp.float32)
    return r[:, :columns] + r[:, columns:]


def power(a, n):
    result = None
    while n:
        if n & 1:
            result = a if result is None else result * a
        a, n = a * a, n >> 1
    return result


def plane_kernel(a_ref, left_ref, right_ref, o_ref):
    left = left_factor(left_ref[...])
    right = right_factor(right_ref[...])

    def one(x, carry):
        o_ref[0, x] = left_product(left, right_product(a_ref[0, x], right))
        return carry

    lax.fori_loop(0, a_ref.shape[1], one, 0, unroll=4)


def plane_transform(a, left, right):
    steps, rows, size_y, size_z = a.shape
    block = pl.BlockSpec((1, rows, size_y, size_z), lambda t: (t, 0, 0, 0))
    whole = lambda m: pl.BlockSpec(m.shape, lambda t: (0, 0))
    return pl.pallas_call(
        plane_kernel,
        grid=(steps,),
        in_specs=[block, whole(left), whole(right)],
        out_specs=block,
        out_shape=jax.ShapeDtypeStruct(a.shape, jnp.float32),
        compiler_params=pltpu.CompilerParams(vmem_limit_bytes=60 * 2**20),
    )(a, left, right)


def spans(sizes):
    starts = [sum(sizes[:i]) for i in range(len(sizes))]
    return list(zip(starts, sizes))


def growing(total):
    if total % 256:
        return [total]
    return [total // 256 * share for share in (8, 56, 192)]


def shrinking(total):
    if total % 256:
        return [total]
    return [total // 256 * share for share in (160, 64, 32)]


def transform_planes(source, target, start, count, left, right, shift=0):
    def one(u, carry):
        target[u - shift] = left_product(left, right_product(source[u], right))
        return carry

    lax.fori_loop(start, start + count, one, 0, unroll=8 if count % 8 == 0 else 1)


def messages(chunks, total):
    outward = [(0, *s) for s in spans(growing(total))]
    outward += [(c, 0, total) for c in range(1, chunks)]
    homeward = [(c, 0, total) for c in range(chunks - 1)]
    homeward += [(chunks - 1, *s) for s in spans(shrinking(total))]
    return outward, homeward


def fused_kernel(
    space_count, time_count, chunks, rows,
    in_ref, vx_ref, vy_ref, vz_ref, ex_ref, ey_ref, ez_ref, out_ref,
    send, recv, fins, matrices, values, ex, shift,
    load_sem, matrix_sem, value_sem, own_in, own_out,
    go_send, go_recv, back_send, back_recv, st_send, st_recv,
):
    total, band_rows = recv.shape[2], recv.shape[3]
    size_x, size_z = fins.shape[3], fins.shape[4]
    size_y = vy_ref.shape[0]
    steps = total // rows
    band = band_rows * chunks
    me = lax.axis_index("space")
    position = lax.axis_index("tm")
    outward, homeward = messages(chunks, total)
    middle = space_count // 2
    offsets = sorted(range(1, space_count), key=lambda k: abs(k - middle))

    def peer_of(k):
        return lax.rem(me + k, space_count)

    def timer_of(k):
        return lax.rem(position + k, time_count)

    def columns(owner, c):
        return pl.ds(pl.multiple_of(owner * band + c * band_rows, tile_rows), band_rows)

    def go(g, peer, slot):
        c, start, count = outward[g]
        return pltpu.make_async_remote_copy(
            src_ref=send.at[pl.ds(start, count), columns(peer, c), :],
            dst_ref=recv.at[c, slot, pl.ds(start, count)],
            send_sem=go_send.at[g, peer],
            recv_sem=go_recv.at[g, slot],
            device_id={"space": peer},
            device_id_type=pl.DeviceIdType.MESH,
        )

    def back(g, peer, slot):
        c, start, count = homeward[g]
        return pltpu.make_async_remote_copy(
            src_ref=recv.at[c, peer, pl.ds(start, count)],
            dst_ref=out_ref.at[pl.ds(start, count), columns(slot, c), :],
            send_sem=back_send.at[g, peer],
            recv_sem=back_recv.at[g, slot],
            device_id={"space": peer},
            device_id_type=pl.DeviceIdType.MESH,
        )

    def final(c, peer, owner):
        return pltpu.make_async_remote_copy(
            src_ref=fins.at[c, owner],
            dst_ref=fins.at[c, owner],
            send_sem=st_send.at[c, peer],
            recv_sem=st_recv.at[c, owner],
            device_id={"tm": peer},
            device_id_type=pl.DeviceIdType.MESH,
        )

    def take_own(g):
        c, start, count = outward[g]
        return pltpu.make_async_copy(
            send.at[pl.ds(start, count), columns(me, c), :],
            recv.at[c, me, pl.ds(start, count)],
            own_in.at[g],
        )

    def give_own(g):
        c, start, count = homeward[g]
        return pltpu.make_async_copy(
            recv.at[c, me, pl.ds(start, count)],
            out_ref.at[pl.ds(start, count), columns(me, c), :],
            own_out.at[g],
        )

    loads = [
        pltpu.make_async_copy(
            in_ref.at[pl.ds(start, count)], send.at[pl.ds(start, count)], load_sem.at[g]
        )
        for g, (start, count) in enumerate(spans(growing(total)))
    ]
    fetches = [
        pltpu.make_async_copy(ref, matrices.at[i], matrix_sem.at[i])
        for i, ref in enumerate((vz_ref, vy_ref, vx_ref))
    ]
    fetches += [
        pltpu.make_async_copy(ref, values.at[i], value_sem.at[i])
        for i, ref in enumerate((ex_ref, ey_ref, ez_ref))
    ]
    barrier = pltpu.get_barrier_semaphore()
    for k in range(1, space_count):
        pl.semaphore_signal(
            barrier, inc=1, device_id={"space": peer_of(k)}, device_id_type=pl.DeviceIdType.MESH
        )
    for k in range(1, time_count):
        pl.semaphore_signal(
            barrier, inc=1, device_id={"tm": timer_of(k)}, device_id_type=pl.DeviceIdType.MESH
        )
    for copy in fetches[:2] + loads + fetches[2:]:
        copy.start()

    fetches[0].wait()
    right = right_factor(matrices[0])
    fetches[1].wait()
    left = left_factor(matrices[1].T)
    for g, (c, start, count) in enumerate(outward):
        if c == 0:
            loads[g].wait()
            transform_planes(send, send, start, count, left, right)
        if g == 0:
            pl.semaphore_wait(barrier, space_count + time_count - 2)
        for k in offsets:
            go(g, peer_of(k), me).start()
        take_own(g).start()

    for copy in fetches[2:]:
        copy.wait()
    ex[...] = jnp.broadcast_to(values[0], (size_z, size_x)).T
    shift[...] = jnp.broadcast_to(values[1], (size_z, size_y)).T + values[2]
    left = left_factor(matrices[2].T)
    left_back = left_factor(matrices[2])

    def view(c, s, t):
        return recv.at[c, s, pl.ds(t * rows, rows)].reshape(rows * band_rows, size_z)

    def load(c, t, j):
        parts = [view(c, s, t)[pl.ds(j, rows, stride=band_rows), :] for s in range(space_count)]
        return jnp.concatenate(parts, axis=0)

    def store(c, t, j, value):
        for s in range(space_count):
            view(c, s, t)[pl.ds(j, rows, stride=band_rows), :] = value[s * rows : (s + 1) * rows]

    def damping_of(c, j):
        row = shift[pl.ds(me * band + c * band_rows + j, 1), :]
        return 1.0 / (1.0 + (ex[...] + row))

    for c in range(chunks):
        for g in range(len(outward)):
            if outward[g][0] == c:
                for k in offsets:
                    go(g, peer_of(k), peer_of(k)).wait_recv()
                take_own(g).wait()

        def forward_mode(j, carry, c=c):
            damping = damping_of(c, j)

            def forward(t, state):
                state = damping * (state + left_product(left, load(c, t, j)))
                store(c, t, j, state)
                return state

            fins[c, position, j] = lax.fori_loop(
                0, steps, forward, jnp.zeros_like(damping), unroll=2
            )
            return carry

        lax.fori_loop(0, band_rows, forward_mode, 0)
        for k in range(1, time_count):
            final(c, timer_of(k), position).start()
        for k in range(1, time_count):
            final(c, timer_of(k), timer_of(k)).wait_recv()

        def inverse_mode(j, carry, c=c):
            damping = damping_of(c, j)
            block_decay = power(damping, steps)
            overall = fins[c, 0, j]
            for p in range(1, time_count):
                overall = block_decay * overall + fins[c, p, j]
            incoming = (circulant_alpha * overall) / (
                1.0 - circulant_alpha * power(block_decay, time_count)
            )
            for p in range(time_count - 1):
                incoming = jnp.where(
                    p < position, block_decay * incoming + fins[c, p, j], incoming
                )

            def inverse(t, incoming):
                incoming = damping * incoming
                store(c, t, j, left_product(left_back, load(c, t, j) + incoming))
                return incoming

            lax.fori_loop(0, steps, inverse, incoming, unroll=2)
            return carry

        lax.fori_loop(0, band_rows, inverse_mode, 0)
        for g in range(len(homeward)):
            if homeward[g][0] == c:
                for k in offsets:
                    back(g, peer_of(k), me).start()
                give_own(g).start()

    left = left_factor(matrices[1])
    right = right_factor(matrices[0].T)
    for g, (c, start, count) in enumerate(homeward):
        for k in offsets:
            back(g, peer_of(k), peer_of(k)).wait_recv()
        give_own(g).wait()
        if c == chunks - 1 and g < len(homeward) - 1:
            transform_planes(out_ref, out_ref, start, count, left, right)

    for c in range(chunks):
        for k in range(1, time_count):
            final(c, timer_of(k), position).wait_send()
    for g in range(len(outward)):
        for k in offsets:
            go(g, peer_of(k), me).wait_send()
    for g in range(len(homeward)):
        for k in offsets:
            back(g, peer_of(k), me).wait_send()


def closing_kernel(in_ref, left_ref, right_ref, out_ref, last, sems):
    held = last.shape[0]
    done = in_ref.shape[0] - held
    pieces = sems.shape[0] - 1
    piece = done // pieces
    copies = [
        pltpu.make_async_copy(
            in_ref.at[pl.ds(i * piece, piece)], out_ref.at[pl.ds(i * piece, piece)], sems.at[i]
        )
        for i in range(pieces)
    ]
    for copy in copies:
        copy.start()
    left = left_factor(left_ref[...])
    right = right_factor(right_ref[...].T)
    transform_planes(in_ref, last, done, held, left, right, shift=done)
    copies.append(pltpu.make_async_copy(last, out_ref.at[pl.ds(done, held)], sems.at[pieces]))
    copies[-1].start()
    for copy in copies:
        copy.wait()


def close(planes, left, right):
    vmem = pl.BlockSpec(memory_space=pltpu.VMEM)
    held = shrinking(planes.shape[0])[-1]
    done = planes.shape[0] - held
    pieces = 7 if done % 7 == 0 else 1
    return pl.pallas_call(
        closing_kernel,
        in_specs=[vmem] * 3,
        out_specs=pl.BlockSpec(memory_space=pltpu.HBM),
        out_shape=jax.ShapeDtypeStruct(planes.shape, jnp.float32),
        scratch_shapes=[
            pltpu.VMEM((held, *planes.shape[1:]), jnp.float32),
            pltpu.SemaphoreType.DMA((pieces + 1,)),
        ],
        compiler_params=pltpu.CompilerParams(vmem_limit_bytes=24 * 2**20),
    )(planes, left, right)


def fused_solve(field, eigvec_x, eigvec_y, eigvec_z, eigval_x, eigval_y, eigval_z):
    space_count = lax.axis_size("space")
    time_count = lax.axis_size("tm")
    steps, rows, size_y, size_z = field.shape
    planes = field.reshape(steps * rows, size_y, size_z)
    band = size_y // space_count
    chunks = 2 if band % (2 * tile_rows) == 0 else 1
    band_rows = band // chunks
    size_x = rows * space_count
    outward, homeward = messages(chunks, steps * rows)
    vmem = pl.BlockSpec(memory_space=pltpu.VMEM)
    hbm = pl.BlockSpec(memory_space=pl.ANY)
    dma = pltpu.SemaphoreType.DMA
    f32 = jnp.float32
    update = pl.pallas_call(
        functools.partial(fused_kernel, space_count, time_count, chunks, rows),
        in_specs=[hbm] * 7,
        out_specs=vmem,
        out_shape=pltpu.VMEM(planes.shape, f32),
        scratch_shapes=[
            pltpu.VMEM(planes.shape, f32),
            pltpu.VMEM((chunks, space_count, steps * rows, band_rows, size_z), f32),
            pltpu.VMEM((chunks, time_count, band_rows, size_x, size_z), f32),
            pltpu.VMEM((3, size_y, size_z), f32),
            pltpu.VMEM((3, 1, size_z), f32),
            pltpu.VMEM((size_x, size_z), f32),
            pltpu.VMEM((size_y, size_z), f32),
            dma((len(growing(steps * rows)),)),
            dma((3,)),
            dma((3,)),
            dma((len(outward),)),
            dma((len(homeward),)),
            dma((len(outward), space_count)),
            dma((len(outward), space_count)),
            dma((len(homeward), space_count)),
            dma((len(homeward), space_count)),
            dma((chunks, time_count)),
            dma((chunks, time_count)),
        ],
        compiler_params=pltpu.CompilerParams(
            collective_id=0, has_side_effects=True, vmem_limit_bytes=44 * 2**20
        ),
    )(
        planes,
        eigvec_x,
        eigvec_y,
        eigvec_z,
        eigval_x.reshape(1, -1),
        eigval_y.reshape(1, -1),
        eigval_z.reshape(1, -1),
    )
    return close(update, eigvec_y, eigvec_z).reshape(field.shape)


def entering(part, axis, combine, identity):
    place = lax.axis_index(axis)
    gathered = jax.tree.map(lambda a: lax.all_gather(a, axis), part)
    state = jax.tree.map(lambda a, e: jnp.zeros_like(a) + jnp.asarray(e, a.dtype), part, identity)

    def one(step, state):
        return combine(
            state, jax.tree.map(lambda a: lax.dynamic_index_in_dim(a, step, 0, False), gathered)
        )

    return lax.fori_loop(0, place, one, state)


def recurrence_solve(values, shifts, time_count):
    steps_local = values.shape[0]
    damping = 1.0 / (1.0 + shifts)

    def advance(running, step_row):
        running = damping * (running + step_row)
        return (running, running)

    final_state, partial_value = lax.scan(advance, jnp.zeros_like(shifts), values)
    block_decay = damping**steps_local
    position = lax.axis_index("tm")

    def compose(early_map, late_map):
        return (early_map[0] * late_map[0], late_map[0] * early_map[1] + late_map[1])

    lead_power, offset = entering(
        (block_decay, final_state), "tm", compose, (jnp.ones_like(shifts), jnp.zeros_like(shifts))
    )
    tail_power = jnp.power(block_decay, (time_count - 1 - position).astype(jnp.float32))
    overall = lax.psum(tail_power * final_state, "tm")
    start_value = circulant_alpha * overall / (1.0 - circulant_alpha * block_decay**time_count)
    incoming = lead_power * start_value + offset
    exponents = jnp.arange(1, steps_local + 1, dtype=jnp.int32).astype(jnp.float32)
    powers = jnp.power(damping[None], exponents[:, None, None])
    return partial_value + powers * incoming[None]


def narrow_solve(planes, eigvec_x, eigval_x, shift_yz, time_count):
    steps_local, rows_x, size_y, size_z = planes.shape
    planes = planes.reshape(steps_local, rows_x, size_y * size_z)
    x_lines = lax.all_to_all(planes, "space", split_axis=2, concat_axis=1, tiled=True)
    x_lines = jnp.einsum("txm,xi->tim", x_lines, eigvec_x, precision=highest)
    shifts = eigval_x[:, None] + shift_yz.reshape(1, -1)
    x_lines = recurrence_solve(x_lines, shifts, time_count)
    x_lines = jnp.einsum("tim,xi->txm", x_lines, eigvec_x, precision=highest)
    planes = lax.all_to_all(x_lines, "space", split_axis=1, concat_axis=2, tiled=True)
    return planes.reshape(steps_local, rows_x, size_y, size_z)


def fits(field, space_count, time_count):
    steps, rows, size_y, size_z = field.shape
    band = size_y // space_count
    if band % tile_rows or rows % tile_rows or not rows * space_count == size_y == size_z or steps * rows % 256:
        return False
    states = (time_count + 1) * band * rows * space_count * size_z
    return 4 * (3 * field.size + states) < 60 * 2**20


def shards(residual_field, eigvec_x, eigvec_y, eigvec_z, eigval_x, eigval_y, eigval_z):
    size_y = residual_field.shape[2]
    space_count = lax.axis_size("space")
    time_count = lax.axis_size("tm")
    if fits(residual_field, space_count, time_count):
        return fused_solve(
            residual_field, eigvec_x, eigvec_y, eigvec_z, eigval_x, eigval_y, eigval_z
        )
    planes = plane_transform(residual_field, eigvec_y.T, eigvec_z)
    band = size_y // space_count
    shift_y = lax.dynamic_slice_in_dim(eigval_y, lax.axis_index("space") * band, band, 0)
    shift_yz = shift_y[:, None] + eigval_z[None, :]
    planes = narrow_solve(planes, eigvec_x, eigval_x, shift_yz, time_count)
    return plane_transform(planes, eigvec_y, eigvec_z.T)


def solution(mesh):
    placed = (P("tm", "space", None, None), P(), P(), P(), P(), P(), P())
    return jax.shard_map(
        shards, mesh=mesh, in_specs=placed, out_specs=P("tm", "space", None, None), check_vma=False
    )
```
